32 devices in a mesh: gy: 8 (over y, x, core), gz: 4 (over z).
Axes of the slice: x: 2, y: 2, z: 4, core: 2. Of those that a mesh axis runs over, the one named last changes fastest.
Arguments:
- start_block: float32 [16, 64, 128, 128], P(None, 'gy', 'gz'), may hold values from -6 to 6
- diagonal: float32 [64, 128, 128], P('gy', 'gz'), may hold values from 0.25 to 4
- gaussian: float32 [512, 128], replicated, may hold values from -0.5 to 0.5
- bucket: int32 [64, 128], P('gy', 'gz'), may hold values from 0 to 3
- flip: int32 [64, 128], P('gy', 'gz'), may hold values from 0 to 1
Outputs:
- basis: float32 [16, 64, 128, 128], P(None, 'gy', 'gz')
- alphas: float32 [3, 16, 16], replicated
- factors: float32 [3, 16, 16], replicated
The draws below stay inside these ranges and needn't reach their ends.
All inputs are finite; a program needn't handle non-finite values.
Results may differ from the reference program's by a relative error of at most 0.0003.
Values sent between devices are 32-bit elements; how exact they have to be, the bound alone decides.
No kernel may reach another device: no remote copies, remote signals or barrier semaphores. Data moves between devices by JAX's collectives and lax.ppermute only.
A program may use at most 64 MiB of HBM per device.

```python
import math
import jax
import jax.numpy as jnp
from jax import lax

NX = 128
BLOCK = 16
SKETCH = 512
BUCKETS = 4
ITERS = 3
NY = 64
NZ = 128


def plant(array, own_key, smallest, high):
    shape = array.shape
    index_at = [jax.random.randint(jax.random.fold_in(own_key, axis), (), 0, shape[axis]) for axis in range(len(shape))]
    array = array.at[tuple(index_at)].set(smallest)
    longest = shape.index(max(shape))
    index_at[longest] = (index_at[longest] + 1) % shape[longest]
    return array.at[tuple(index_at)].set(high)


def shard_levels(own_key, extent, cuts, least, high):
    level, own = 1.0, jax.random.fold_in(own_key, 6)
    for position, parts in cuts:
        draws = jnp.exp(jax.random.uniform(jax.random.fold_in(own, position), (parts,), jnp.float32, least / len(cuts), high / len(cuts)))
        level = level * jnp.repeat(draws, extent[position] // parts).reshape([-1 if axis == position else 1 for axis in range(len(extent))])
    return level


def scatter_about(own_key, shape, spread, limit, split=(), kind=jnp.bfloat16):
    values = spread * jax.random.normal(own_key, shape, jnp.float32)
    if split:
        values = values * shard_levels(own_key, shape, split, -0.22, 0.18)
    return jnp.clip(values, -limit, limit).astype(kind)


def setup_inputs(seed: int = 0) -> dict:
    arg_keys = jax.random.split(jax.random.key(seed), 6)
    start_block = scatter_about(arg_keys[0], (BLOCK, NY, NZ, NX), 1.0, 6.0, ((1, 8), (2, 4)), jnp.float32)
    diagonal = jnp.clip(jnp.exp(math.log(4.0) - 2.7725887 * jax.random.uniform(arg_keys[1], (NY, NZ, NX), jnp.float32) ** shard_levels(arg_keys[1], (NY, NZ, NX), ((0, 8), (1, 4)), -0.2, 0.2)), 0.25, 4.0)
    gaussian = scatter_about(arg_keys[2], (SKETCH, NX), (SKETCH // BUCKETS) ** -0.5, 0.5, (), jnp.float32)
    bucket = plant(jax.random.randint(arg_keys[3], (NY, NZ), 0, BUCKETS), jax.random.fold_in(arg_keys[3], 1), 0, BUCKETS - 1).astype(jnp.int32)
    flip = plant(jax.random.randint(arg_keys[4], (NY, NZ), 0, 2), jax.random.fold_in(arg_keys[4], 1), 0, 1).astype(jnp.int32)
    return dict(start_block=start_block, diagonal=diagonal, gaussian=gaussian, bucket=bucket, flip=flip)


HIGH = lax.Precision.HIGHEST

def stencil(field, diagonal):
    padded = jnp.pad(field, 1)
    beside = padded[2:, 1:-1, 1:-1] + padded[:-2, 1:-1, 1:-1]
    beside = beside + padded[1:-1, 2:, 1:-1] + padded[1:-1, :-2, 1:-1]
    beside = beside + padded[1:-1, 1:-1, 2:] + padded[1:-1, 1:-1, :-2]
    return (6.0 + diagonal) * field - beside

def column_weights(bucket, flip):
    labels = bucket.reshape(-1)
    signs = (1 - 2 * flip.reshape(-1)).astype(jnp.float32)
    levels = jnp.arange(BUCKETS, dtype=jnp.int32)
    return (labels[None, :] == levels[:, None]).astype(jnp.float32) * signs[None, :]

def sketch_of(block, weights, pieces, scale):
    columns = block.reshape(block.shape[0], -1, block.shape[3])
    summed = jnp.einsum('kc,bcx->kbx', weights, columns, precision=HIGH)
    sketched = jnp.einsum('krx,kbx->bkr', pieces, summed, precision=HIGH)
    return sketched.reshape(block.shape[0], -1) * scale

def normalize(raw, raw_sketch):
    gram = jnp.dot(raw_sketch, raw_sketch.T, precision=HIGH)
    lower = jnp.linalg.cholesky(gram)
    identity = jnp.eye(raw.shape[0], dtype=jnp.float32)
    inverse = lax.linalg.triangular_solve(lower, identity, left_side=True, lower=True)
    basis = jnp.tensordot(inverse, raw, axes=1, precision=HIGH)
    return (basis, jnp.dot(inverse, raw_sketch, precision=HIGH), lower)

def reference(start_block, diagonal, gaussian, bucket, flip):
    weights = column_weights(bucket, flip)
    pieces = gaussian.reshape(BUCKETS, SKETCH // BUCKETS, NX)
    scale = 1.0 / math.sqrt(NX * NY * NZ)
    basis, sketch, lower = normalize(start_block, sketch_of(start_block, weights, pieces, scale))
    previous = jnp.zeros_like(basis)
    previous_sketch = jnp.zeros_like(sketch)
    alpha_list = []
    factor_list = []
    for number in range(ITERS):
        image = lax.map(lambda field: stencil(field, diagonal), basis)
        image_sketch = sketch_of(image, weights, pieces, scale)
        alpha = jnp.dot(sketch, image_sketch.T, precision=HIGH)
        gamma = jnp.dot(previous_sketch, image_sketch.T, precision=HIGH)
        residual = image - jnp.tensordot(alpha.T, basis, axes=1, precision=HIGH)
        residual = residual - jnp.tensordot(gamma.T, previous, axes=1, precision=HIGH)
        residual_sketch = image_sketch - jnp.dot(alpha.T, sketch, precision=HIGH) - jnp.dot(gamma.T, previous_sketch, precision=HIGH)
        previous, previous_sketch = (basis, sketch)
        basis, sketch, lower = normalize(residual, residual_sketch)
        alpha_list.append(alpha)
        factor_list.append(lower)
    return (basis, jnp.stack(alpha_list), jnp.stack(factor_list))
```

```python
import functools
import math

import jax
import jax.numpy as jnp
from jax import lax
from jax.experimental import pallas as pl
from jax.experimental.pallas import tpu as pltpu
from jax.sharding import PartitionSpec as P

BUCKETS = 4
ITERS = 3
CENTRE = 8.125
AXES = ("gy", "gz")
HIGH = lax.Precision.HIGHEST
VMEM = pltpu.MemorySpace.VMEM
HBM = pltpu.MemorySpace.HBM
MIB = 1 << 20


def call(body, name, outs, ins, scratch=(), limit=16):
    return pl.pallas_call(
        body,
        out_shape=[jax.ShapeDtypeStruct(shape, kind) for shape, kind, _ in outs],
        in_specs=[pl.BlockSpec(memory_space=space) for space in ins],
        out_specs=[pl.BlockSpec(memory_space=space) for _, _, space in outs],
        scratch_shapes=list(scratch),
        compiler_params=pltpu.CompilerParams(vmem_limit_bytes=limit * MIB),
        name=name,
    )


def odd(axis):
    return lax.axis_index(axis) % 2 == 1


def pairs(axis, first):
    size = lax.axis_size(axis)
    swap = {}
    for i in range(first, size - 1 + first, 2):
        swap[i % size], swap[(i + 1) % size] = (i + 1) % size, i % size
    return sorted(swap.items())


def swapped(axis, within, across):
    return lax.ppermute(within, axis, pairs(axis, 0)), lax.ppermute(across, axis, pairs(axis, 1))


def edge(axis):
    index = lax.axis_index(axis)
    return index == 0, index == lax.axis_size(axis) - 1


def when_sides(axis, act):
    @pl.when(odd(axis))
    def _():
        act(0, 1)

    @pl.when(jnp.logical_not(odd(axis)))
    def _():
        act(1, 0)


def small_y(diag, bucket, flip, code_out, within, across):
    ny, nz, _ = diag.shape
    code = (bucket[...] + 1).astype(jnp.float32) * (1 - 2 * flip[...]).astype(jnp.float32)
    code_out[...] = jnp.zeros_like(code_out)
    code_out[:, 0:nz] = code

    def pack(out, low):
        if low:
            layers, rows = diag[0:2], code_out[0:3]
        else:
            layers, rows = diag[ny - 2 : ny], code_out[ny - 3 : ny]
        out[0 : 2 * nz] = layers.reshape(2 * nz, layers.shape[2])
        out[2 * nz : 2 * nz + 8] = jnp.zeros_like(out[2 * nz : 2 * nz + 8])
        out[2 * nz : 2 * nz + 3] = rows

    def act(side_within, side_across):
        pack(within, side_within == 0)
        pack(across, side_across == 0)

    when_sides("gy", act)


def turned(v, vt, ny, nz):
    count = v.shape[0] // (ny * nz)

    def move(col, carry):
        vt[col] = v[pl.ds(col, count, stride=ny * nz), :]
        return carry

    lax.fori_loop(0, ny * nz, move, 0, unroll=16)


def pack_y(vt, after, within, across, ny, nz):
    def act(side_within, side_across):
        for out, side in ((within, side_within), (across, side_across)):
            out[...] = vt[0 : 3 * nz] if side == 0 else vt[(ny - 3) * nz : ny * nz]

    when_sides("gy", act)


def small_z(diag, code, got_within, got_across, codes_out, within, across):
    ny, nz, width = diag.shape
    codes_out[...] = jnp.zeros_like(codes_out)
    codes_out[3 : 3 + ny] = code[...]

    def gather(side_within, side_across):
        for got, side, at_edge in zip(
            (got_within, got_across), (side_within, side_across), ("w", "a")
        ):
            start = 0 if side == 0 else 3 + ny
            wrapped = edge("gy")[side]
            rows = got[2 * nz : 2 * nz + 3]
            codes_out[start : start + 3] = jnp.where(wrapped, jnp.zeros_like(rows), rows)

    when_sides("gy", gather)
    y_low_within = odd("gy")

    def pack(out, low):
        z0 = 0 if low else nz - 2
        for t in range(2):
            for y in range(ny):
                out[(y + 2) * 2 + t : (y + 2) * 2 + t + 1] = diag[y, z0 + t : z0 + t + 1]
            for layer in range(2):
                row = layer * nz + z0 + t
                a = got_within[row : row + 1]
                b = got_across[row : row + 1]
                out[layer * 2 + t : layer * 2 + t + 1] = jnp.where(y_low_within, a, b)
                high = (ny + 2 + layer) * 2 + t
                out[high : high + 1] = jnp.where(y_low_within, b, a)
        base = 2 * (ny + 4)
        c0 = 0 if low else nz - 3
        out[base : base + 16] = jnp.zeros_like(out[base : base + 16])
        out[base : base + 16, 0:3] = codes_out[:, c0 : c0 + 3]

    def act(side_within, side_across):
        pack(within, side_within == 0)
        pack(across, side_across == 0)

    when_sides("gz", act)


def spread_diagonal(dr, diag, y_within, y_across, z_within, z_across):
    ny, nz, width = diag.shape
    shift = 6.0 - CENTRE

    def put(y, z, row):
        dr[y, z] = jnp.broadcast_to(row + shift, (8, width))

    for y in range(ny):
        for z in range(nz):
            put(y + 2, z + 2, diag[y, z : z + 1])

    def y_sides(side_within, side_across):
        for got, side in ((y_within, side_within), (y_across, side_across)):
            start = 0 if side == 0 else ny + 2
            for layer in range(2):
                for z in range(nz):
                    row = layer * nz + z
                    put(start + layer, z + 2, got[row : row + 1])

    def z_sides(side_within, side_across):
        for got, side in ((z_within, side_within), (z_across, side_across)):
            start = 0 if side == 0 else nz + 2
            for y in range(ny + 4):
                for t in range(2):
                    put(y, start + t, got[2 * y + t : 2 * y + t + 1])

    when_sides("gy", y_sides)
    when_sides("gz", z_sides)


def stencil(source, target, dr, ys, zs, source_at, target_at):
    half, width = 8, source.shape[3]
    lane = lax.broadcasted_iota(jnp.int32, (half, width), 1)
    first, last = lane == 0, lane == width - 1

    def row(i, carry):
        sy, ty, dy = i + (ys[0] + source_at), i + (ys[0] + target_at), i + (ys[0] + 2)
        for z in range(zs[0], zs[1]):
            sz, tz = z + source_at, z + target_at
            weight = dr[dy, z + 2]
            for h in range(0, source.shape[2], half):
                part = pl.ds(h, half)
                here = source[sy, sz, part]
                around = source[sy - 1, sz, part] + source[sy + 1, sz, part]
                around = around + (source[sy, sz - 1, part] + source[sy, sz + 1, part])
                left = jnp.where(first, 0.0, pltpu.roll(here, 1, 1))
                right = jnp.where(last, 0.0, pltpu.roll(here, width - 1, 1))
                target[ty, tz, part] = weight * here - (around + (left + right))
        return carry

    lax.fori_loop(0, ys[1] - ys[0], row, 0)


def clear_edges(field, ny, nz, at, reach):
    y_low, y_high = edge("gy")
    z_low, z_high = edge("gz")
    for flag, y in ((y_low, -1), (y_high, ny)):

        @pl.when(flag)
        def _():
            for z in range(-reach, nz + reach):
                field[y + at, z + at] = jnp.zeros(field.shape[2:], field.dtype)

    for flag, z in ((z_low, -1), (z_high, nz)):

        @pl.when(flag)
        def _():
            for y in range(-reach, ny + reach):
                field[y + at, z + at] = jnp.zeros(field.shape[2:], field.dtype)


def weights_to_scalars(codes, z_within, z_across, table, scalars, sem, ny, nz):
    base = 2 * (ny + 4)
    z_low, z_high = edge("gz")
    low_within = odd("gz")
    a = z_within[base : base + 16]
    b = z_across[base : base + 16]
    low = jnp.where(z_low, 0.0, jnp.where(low_within, a, b))
    high = jnp.where(z_high, 0.0, jnp.where(low_within, b, a))
    lane = lax.broadcasted_iota(jnp.int32, (16, 128), 1)
    whole = jnp.where(
        lane < 3,
        low,
        jnp.where(
            lane < nz + 3,
            pltpu.roll(codes[...], 3, 1),
            jnp.where(lane < nz + 6, pltpu.roll(high, nz + 3, 1), 0.0),
        ),
    )
    sign = jnp.where(whole > 0, 1.0, -1.0)
    for k in range(BUCKETS):
        weight = jnp.where(jnp.abs(whole) == k + 1, sign, 0.0)
        table[16 * k : 16 * k + 16] = weight
        beside = pltpu.roll(weight, 1, 1) + pltpu.roll(weight, 127, 1)
        beside = beside + pltpu.roll(weight, 1, 0) + pltpu.roll(weight, 15, 0)
        at = 16 * (BUCKETS + k)
        table[at : at + 16] = beside
    copy = pltpu.make_async_copy(table, scalars, sem)
    copy.start()
    return copy


def local_sketches(
    vt, diag, code, y_within, y_across, z_within, z_across, gaussian, keep_out, give_out,
    e0, e1, e2, dr, table, scalars, sums, sem,
):
    ny, nz, width = diag.shape
    count = vt.shape[1]
    copy = weights_to_scalars(code, z_within, z_across, table, scalars, sem, ny, nz)
    spread_diagonal(dr, diag, y_within, y_across, z_within, z_across)
    e0[...] = jnp.zeros_like(e0)
    e1[...] = jnp.zeros_like(e1)
    for y in range(ny):
        e0[y + 2, 2 : 2 + nz] = vt[y * nz : (y + 1) * nz]
    copy.wait()
    blank = tuple(jnp.zeros((count, width), jnp.float32) for _ in range(BUCKETS))

    def total(field, level, at):
        def row(i, acc):
            acc = list(acc)
            for z in range(-level, nz + level):
                value = field[i + (at - level), z + at]
                for k in range(BUCKETS):
                    weight = scalars[i + (16 * k + 3 - level), z + 3]
                    acc[k] = acc[k] + weight * value
            return tuple(acc)

        acc = lax.fori_loop(0, ny + 2 * level, row, blank)
        for k in range(BUCKETS):
            sums[k, level * count : (level + 1) * count] = acc[k]
        return acc

    def applied(field, level, at):
        def row(i, acc):
            acc = list(acc)
            for z in range(-level, nz + level):
                value = field[i + (at - level), z + at]
                weight = dr[i + (2 - level), z + 2]
                for k in range(BUCKETS):
                    here = scalars[i + (16 * k + 3 - level), z + 3]
                    beside = scalars[i + (16 * (BUCKETS + k) + 3 - level), z + 3]
                    both = weight * here - beside
                    acc[k] = acc[k] + jnp.concatenate([both, both], axis=0) * value
            return tuple(acc)

        return lax.fori_loop(0, ny + 2 * level, row, blank)

    total(e0, 0, 2)
    stencil(e0, e1, dr, (-1, ny + 1), (-1, nz + 1), 2, 3)
    total(e1, 1, 3)
    clear_edges(e1, ny, nz, 3, 1)
    stencil(e1, e2, dr, (-2, ny + 2), (-2, nz + 2), 3, 2)
    last = total(e2, 2, 2)
    clear_edges(e2, ny, nz, 2, 2)
    higher = applied(e2, 2, 2)
    lane = lax.broadcasted_iota(jnp.int32, (count, width), 1)
    for k in range(BUCKETS):
        left = jnp.where(lane == 0, 0.0, pltpu.roll(last[k], 1, 1))
        right = jnp.where(lane == width - 1, 0.0, pltpu.roll(last[k], width - 1, 1))
        sums[k, 3 * count : 4 * count] = higher[k] - (left + right)
    rows = gaussian.shape[0] // BUCKETS

    def part(k):
        return lax.dot_general(
            sums[k],
            gaussian[k * rows : (k + 1) * rows],
            (((1,), (1,)), ((), ())),
            precision=HIGH,
            preferred_element_type=jnp.float32,
        )

    upper = odd("gy")
    size = (ITERS + 1) * count
    for k in range(BUCKETS // 2):
        one, two = part(k), part(k + BUCKETS // 2)
        keep_out[k * size : (k + 1) * size] = jnp.where(upper, two, one)
        give_out[k * size : (k + 1) * size] = jnp.where(upper, one, two)


def pack_z(vt, y_within, y_across, after, within, across, ny, nz):
    def act(side_within, side_across):
        for out, side in ((within, side_within), (across, side_across)):
            z0 = 0 if side == 0 else nz - 3
            for y in range(ny):
                out[y + 3] = vt[y * nz + z0 : y * nz + z0 + 3]

            def corners(low, high):
                for layer in range(3):
                    out[layer] = low[layer * nz + z0 : layer * nz + z0 + 3]
                    out[ny + 3 + layer] = high[layer * nz + z0 : layer * nz + z0 + 3]

            @pl.when(odd("gy"))
            def _():
                corners(y_within, y_across)

            @pl.when(jnp.logical_not(odd("gy")))
            def _():
                corners(y_across, y_within)

    when_sides("gz", act)


def krylov(
    vt, diag, dy_within, dy_across, dz_within, dz_across,
    y_within, y_across, z_within, z_across, high_out, low_out,
    e0, e1, dr, high, low, sems,
):
    ny, nz, width = diag.shape
    count = vt.shape[1]
    spread_diagonal(dr, diag, dy_within, dy_across, dz_within, dz_across)
    for y in range(ny):
        e0[y + 3, 3 : 3 + nz] = vt[y * nz : (y + 1) * nz]
    y_edges, z_edges = edge("gy"), edge("gz")
    blank_y = jnp.zeros((nz, count, width), jnp.float32)
    blank_z = jnp.zeros((3, count, width), jnp.float32)

    def y_sides(side_within, side_across):
        for got, side in ((y_within, side_within), (y_across, side_across)):
            start = 0 if side == 0 else ny + 3
            for layer in range(3):
                e0[start + layer, 3 : 3 + nz] = got[layer * nz : (layer + 1) * nz]

            @pl.when(y_edges[side])
            def _():
                for layer in range(3):
                    e0[start + layer, 3 : 3 + nz] = blank_y

    def z_sides(side_within, side_across):
        for got, side in ((z_within, side_within), (z_across, side_across)):
            start = 0 if side == 0 else nz + 3
            for y in range(ny + 6):
                e0[y, start : start + 3] = got[y]

            @pl.when(z_edges[side])
            def _():
                for y in range(ny + 6):
                    e0[y, start : start + 3] = blank_z

            for y_side in range(2):

                @pl.when(y_edges[y_side])
                def _():
                    for layer in range(3):
                        y = layer if y_side == 0 else ny + 3 + layer
                        e0[y, start : start + 3] = blank_z

    when_sides("gy", y_sides)
    when_sides("gz", z_sides)

    def halves(field, level):
        def row(y, carry):
            for z in range(nz):
                value = field[y + 3, z + 3]
                top = value.astype(jnp.bfloat16)
                rows = pl.ds(level * count, count)
                high[y * nz + z, rows] = top
                low[y * nz + z, rows] = (value - top.astype(jnp.float32)).astype(jnp.bfloat16)
            return carry

        lax.fori_loop(0, ny, row, 0)

    halves(e0, 0)
    stencil(e0, e1, dr, (-2, ny + 2), (-2, nz + 2), 3, 3)
    clear_edges(e1, ny, nz, 3, 2)
    halves(e1, 1)
    stencil(e1, e0, dr, (-1, ny + 1), (-1, nz + 1), 3, 3)
    clear_edges(e0, ny, nz, 3, 1)
    halves(e0, 2)
    stencil(e0, e1, dr, (0, ny), (0, nz), 3, 3)
    halves(e1, 3)
    one = pltpu.make_async_copy(high, high_out, sems.at[0])
    two = pltpu.make_async_copy(low, low_out, sems.at[1])
    one.start()
    two.start()
    one.wait()
    two.wait()


def product(a, b, axis):
    return lax.dot_general(
        a, b, (((1,), (axis,)), ((), ())), precision=HIGH, preferred_element_type=jnp.float32
    )


def factored(gram, block):
    count = gram.shape[0]
    width = 128
    columns = [jnp.broadcast_to(gram[:, j : j + 1], (count, width)) for j in range(count)]
    pieces = [block[:, c : c + width] for c in range(0, block.shape[1], width)]
    row = lax.broadcasted_iota(jnp.int32, (count, width), 0)
    lane = lax.broadcasted_iota(jnp.int32, (count, width), 1)
    lower = jnp.zeros((count, width), jnp.float32)
    scale = jnp.zeros((count, width), jnp.float32)
    for j in range(count):
        pivot = columns[j][j : j + 1]
        root = 1.0 / jnp.sqrt(pivot)
        inverse = root * root
        lower = jnp.where((lane == j) & (row >= j), columns[j] * root, lower)
        scale = jnp.where(row == j, jnp.broadcast_to(root, (count, width)), scale)
        under = jnp.where(row > j, columns[j] * inverse, 0.0)
        for m in range(j + 1, count):
            columns[m] = columns[m] - under * columns[m][j : j + 1]
        pieces = [piece - under * piece[j : j + 1] for piece in pieces]
    return lower, jnp.concatenate([piece * scale for piece in pieces], axis=1)


def finish(kept, got, high_in, low_in, out, alphas, factors, high, low, block, sems, out_sem, ny, nz, scale):
    count = alphas.shape[1]
    size = (ITERS + 1) * count
    width = kept.shape[1]
    one = pltpu.make_async_copy(high_in, high, sems.at[0])
    two = pltpu.make_async_copy(low_in, low, sems.at[1])
    one.start()
    two.start()
    upper = odd("gy")
    first = jnp.where(upper, got[...], kept[...])
    second = jnp.where(upper, kept[...], got[...])
    parts = [first[0:size], first[size:], second[0:size], second[size:]]
    whole = jnp.concatenate(parts, axis=1) * scale
    row = lax.broadcasted_iota(jnp.int32, (count, width), 0)
    lane = lax.broadcasted_iota(jnp.int32, (count, width), 1)
    identity = jnp.where(row == lane, 1.0, 0.0)
    start = whole[0:count]
    lower, current = factored(
        product(start, start, 1), jnp.concatenate([start, identity], axis=1)
    )
    previous = jnp.zeros_like(current)
    span = whole.shape[1]
    for number in range(ITERS):
        raised = pltpu.roll(current[:, span:], count, 1)
        image_sketch = product(raised[:, 0:size], whole, 0)
        image = jnp.concatenate([image_sketch, raised], axis=1) + CENTRE * current
        both = jnp.concatenate([current, previous], axis=0)
        mixed = product(image[:, 0:span], both[:, 0:span], 1)
        alphas[number] = product(current[:, 0:span], image[:, 0:span], 1)
        residual = image - product(mixed, both, 0)
        previous = current
        sketch = residual[:, 0:span]
        lower, current = factored(product(sketch, sketch, 1), residual)
        factors[number] = lower[:, 0:count]
    mix = current[:, span : span + size]
    group = 4
    tiled = jnp.concatenate([mix] * group, axis=1)
    tiled = jnp.concatenate([tiled] * group, axis=0)
    at_row = lax.broadcasted_iota(jnp.int32, tiled.shape, 0) // count
    at_lane = lax.broadcasted_iota(jnp.int32, tiled.shape, 1) // size
    tiled = jnp.where(at_row == at_lane, tiled, 0.0)
    mix_high = tiled.astype(jnp.bfloat16)
    mix_low = (tiled - mix_high.astype(jnp.float32)).astype(jnp.bfloat16)
    one.wait()
    two.wait()

    def dot(a, b):
        return jnp.dot(a, b, preferred_element_type=jnp.float32)

    def copies(y):
        return [
            pltpu.make_async_copy(block.at[y, pl.ds(b * nz, nz)], out.at[b, y], out_sem)
            for b in range(count)
        ]

    def layer(y, carry):
        for z in range(0, nz, group):
            col = y * nz + z
            top = high[pl.ds(col, group)].reshape(group * size, width)
            bottom = low[pl.ds(col, group)].reshape(group * size, width)
            value = dot(mix_high, top) + (dot(mix_high, bottom) + dot(mix_low, top))
            for c in range(group):
                block[y, pl.ds(z + c, count, stride=nz), :] = value[c * count : (c + 1) * count]
        for copy in copies(y):
            copy.start()
        return carry

    lax.fori_loop(0, ny, layer, 0)

    def drain(y, carry):
        for copy in copies(y):
            copy.wait()
        return carry

    lax.fori_loop(0, ny, drain, 0)


def reduced(kept, given):
    ny, nz = lax.axis_size("gy"), lax.axis_size("gz")
    total = ny * nz

    def exchange(value, bit):
        return lax.ppermute(value, AXES, [(i, i ^ bit) for i in range(total)])

    half = kept + exchange(given, nz)
    bit = 1
    while bit < nz:
        half = half + exchange(half, bit)
        bit *= 2
    after = half
    bit = 2 * nz
    while bit < total:
        half = half + exchange(half, bit)
        bit *= 2
    return half, exchange(half, nz), after


def on_device(start_block, diagonal, gaussian, bucket, flip):
    count, ny, nz, width = start_block.shape
    cells = width * ny * lax.axis_size("gy") * nz * lax.axis_size("gz")
    scale = 1.0 / math.sqrt(cells)
    f32, bf16 = jnp.float32, jnp.bfloat16
    size = (ITERS + 1) * count
    small_rows_y = 2 * nz + 8
    small_rows_z = 2 * (ny + 4) + 16
    code, within, across = call(
        small_y, "small_y",
        [((ny, 128), f32, VMEM), ((small_rows_y, width), f32, VMEM), ((small_rows_y, width), f32, VMEM)],
        [VMEM] * 3,
    )(diagonal, bucket, flip)
    dy = swapped("gy", within, across)
    flat = start_block.reshape(count * ny * nz, width)
    side = (3 * nz, count, width)
    (vt,) = call(
        functools.partial(turned, ny=ny, nz=nz), "turned",
        [((ny * nz, count, width), f32, VMEM)],
        [VMEM],
    )(flat)
    codes, within, across = call(
        small_z, "small_z",
        [((16, 128), f32, VMEM), ((small_rows_z, width), f32, VMEM), ((small_rows_z, width), f32, VMEM)],
        [VMEM] * 4,
    )(diagonal, code, *dy)
    dz = swapped("gz", within, across)
    y_halo = swapped(
        "gy",
        *call(
            functools.partial(pack_y, ny=ny, nz=nz), "pack_y",
            [(side, f32, VMEM), (side, f32, VMEM)],
            [VMEM] * 2,
        )(vt, codes),
    )
    half = (BUCKETS // 2 * size, 128)
    field = lambda ring: pltpu.VMEM((ny + 2 * ring, nz + 2 * ring, count, width), f32)
    spread = pltpu.VMEM((ny + 4, nz + 4, 8, width), f32)
    kept, given = call(
        local_sketches, "local_sketches",
        [(half, f32, VMEM), (half, f32, VMEM)],
        [VMEM] * 8,
        [
            field(2), field(3), field(2), spread,
            pltpu.VMEM((32 * BUCKETS, 128), f32), pltpu.SMEM((32 * BUCKETS, 128), f32),
            pltpu.VMEM((BUCKETS, size, width), f32), pltpu.SemaphoreType.DMA,
        ],
        limit=28,
    )(vt, diagonal, codes, *dy, *dz, gaussian)
    kept, got, after = reduced(kept, given)
    z_side = (ny + 6, 3, count, width)
    z_halo = swapped(
        "gz",
        *call(
            functools.partial(pack_z, ny=ny, nz=nz), "pack_z",
            [(z_side, f32, VMEM), (z_side, f32, VMEM)],
            [VMEM] * 4,
        )(vt, *y_halo, after),
    )
    columns = (ny * nz, size, width)
    pair = [pltpu.VMEM(columns, bf16), pltpu.VMEM(columns, bf16)]
    sems = pltpu.SemaphoreType.DMA((2,))
    high, low = call(
        krylov, "krylov",
        [(columns, bf16, HBM), (columns, bf16, HBM)],
        [VMEM] * 10,
        [field(3), field(3), spread, *pair, sems],
        limit=36,
    )(vt, diagonal, *dy, *dz, *y_halo, *z_halo)
    square = (ITERS, count, count)
    basis, alphas, factors = call(
        functools.partial(finish, ny=ny, nz=nz, scale=scale), "finish",
        [(start_block.shape, f32, HBM), (square, f32, VMEM), (square, f32, VMEM)],
        [VMEM, VMEM, HBM, HBM],
        [*pair, pltpu.VMEM((ny, count * nz, width), f32), sems, pltpu.SemaphoreType.DMA],
        limit=28,
    )(kept, got, high, low)
    return basis, alphas, factors


def solution(mesh):
    in_specs = (P(None, "gy", "gz", None), P("gy", "gz", None), P(), P("gy", "gz"), P("gy", "gz"))
    out_specs = (P(None, "gy", "gz", None), P(), P())
    return jax.shard_map(
        on_device, mesh=mesh, in_specs=in_specs, out_specs=out_specs, check_vma=False
    )
```

```python
import functools
import math

import jax
import jax.numpy as jnp
from jax import lax
from jax.experimental import pallas as pl
from jax.experimental.pallas import tpu as pltpu
from jax.sharding import PartitionSpec as P


BUCKETS = 4
ITERS = 3
CENTRE = 8.125
AXES = ("gy", "gz")
HIGH = lax.Precision.HIGHEST
VMEM = pltpu.MemorySpace.VMEM
HBM = pltpu.MemorySpace.HBM
MIB = 1 << 20
WORK = 2 << 30


def call(body, outs, ins, scratch=(), limit=16, cost=0):
    return pl.pallas_call(
        body,
        out_shape=[jax.ShapeDtypeStruct(shape, kind) for shape, kind, _ in outs],
        in_specs=[pl.BlockSpec(memory_space=space) for space in ins],
        out_specs=[pl.BlockSpec(memory_space=space) for _, _, space in outs],
        scratch_shapes=list(scratch),
        cost_estimate=pl.CostEstimate(flops=cost, bytes_accessed=0, transcendentals=0) if cost else None,
        compiler_params=pltpu.CompilerParams(vmem_limit_bytes=limit * MIB),
    )


def odd(axis):
    return lax.axis_index(axis) % 2 == 1


def line(axis):
    ny, nz = lax.axis_size("gy"), lax.axis_size("gz")
    swap = []
    for y in range(ny):
        for z in range(nz):
            place, size = (y, ny) if axis == "gy" else (z, nz)
            ahead = place + 1 if place % 2 else place - 1
            if axis == "gy":
                partner = ahead % ny * nz + z
            elif 0 <= ahead < size:
                partner = y * nz + ahead
            else:
                partner = (y ^ 1) * nz + z
            swap.append((y * nz + z, partner))
    return swap


def swapped(axis, within, across):
    first = lax.ppermute(within, axis, [(i, i ^ 1) for i in range(lax.axis_size(axis))])
    second = lax.ppermute(across, AXES, line(axis))
    return first, second


def edge(axis):
    index = lax.axis_index(axis)
    return index == 0, index == lax.axis_size(axis) - 1


def when_sides(axis, act):
    @pl.when(odd(axis))
    def _():
        act(0, 1)

    @pl.when(jnp.logical_not(odd(axis)))
    def _():
        act(1, 0)


def small_y(diag_in, bucket_in, flip_in, diag, code_out, within, across, bucket, flip, sems):
    copies = [
        pltpu.make_async_copy(source, target, sems.at[i])
        for i, (source, target) in enumerate(((diag_in, diag), (bucket_in, bucket), (flip_in, flip)))
    ]
    for copy in copies:
        copy.start()
    for copy in copies:
        copy.wait()
    ny, nz, _ = diag.shape
    code = (bucket[...] + 1).astype(jnp.float32) * (1 - 2 * flip[...]).astype(jnp.float32)
    code_out[...] = jnp.zeros_like(code_out)
    code_out[:, 0:nz] = code

    def pack(out, low):
        if low:
            layers, rows = diag[0:2], code_out[0:3]
        else:
            layers, rows = diag[ny - 2 : ny], code_out[ny - 3 : ny]
        out[0 : 2 * nz] = layers.reshape(2 * nz, layers.shape[2])
        out[2 * nz : 2 * nz + 8] = jnp.zeros_like(out[2 * nz : 2 * nz + 8])
        out[2 * nz : 2 * nz + 3] = rows

    def act(side_within, side_across):
        pack(within, side_within == 0)
        pack(across, side_across == 0)

    when_sides("gy", act)


def turned(v_in, vt, y_within, y_across, z_within, z_across, v, sems, ny, nz):
    count = vt.shape[1]
    step = v.shape[1] // count

    def copies(y):
        return [
            pltpu.make_async_copy(v_in.at[b, y], v.at[y, pl.ds(b * step, nz)], sems.at[y])
            for b in range(count)
        ]

    for y in range(ny):
        for copy in copies(y):
            copy.start()

    def layer(y, carry):
        for copy in copies(y):
            copy.wait()
        for z in range(nz):
            vt[y * nz + z] = v[y, pl.ds(z, count, stride=step), :]
        return carry

    lax.fori_loop(0, ny, layer, 0)

    def y_sides(side_within, side_across):
        for out, side in ((y_within, side_within), (y_across, side_across)):
            out[...] = vt[0 : 3 * nz] if side == 0 else vt[(ny - 3) * nz : ny * nz]

    def z_sides(side_within, side_across):
        for out, side in ((z_within, side_within), (z_across, side_across)):
            z0 = 0 if side == 0 else nz - 3
            for y in range(ny):
                out[y] = vt[y * nz + z0 : y * nz + z0 + 3]

    when_sides("gy", y_sides)
    when_sides("gz", z_sides)


def small_z(diag, code, got_within, got_across, codes_out, within, across):
    ny, nz, _ = diag.shape
    codes_out[...] = jnp.zeros_like(codes_out)
    codes_out[3 : 3 + ny] = code[...]

    def gather(side_within, side_across):
        for got, side in zip((got_within, got_across), (side_within, side_across)):
            start = 0 if side == 0 else 3 + ny
            wrapped = edge("gy")[side]
            rows = got[2 * nz : 2 * nz + 3]
            codes_out[start : start + 3] = jnp.where(wrapped, jnp.zeros_like(rows), rows)

    when_sides("gy", gather)
    y_low_within = odd("gy")

    def pack(out, low):
        z0 = 0 if low else nz - 2
        for t in range(2):
            for y in range(ny):
                out[(y + 2) * 2 + t : (y + 2) * 2 + t + 1] = diag[y, z0 + t : z0 + t + 1]
            for layer in range(2):
                row = layer * nz + z0 + t
                a = got_within[row : row + 1]
                b = got_across[row : row + 1]
                out[layer * 2 + t : layer * 2 + t + 1] = jnp.where(y_low_within, a, b)
                high = (ny + 2 + layer) * 2 + t
                out[high : high + 1] = jnp.where(y_low_within, b, a)
        base = 2 * (ny + 4)
        c0 = 0 if low else nz - 3
        out[base : base + 16] = jnp.zeros_like(out[base : base + 16])
        out[base : base + 16, 0:3] = codes_out[:, c0 : c0 + 3]

    def act(side_within, side_across):
        pack(within, side_within == 0)
        pack(across, side_across == 0)

    when_sides("gz", act)


def spread_diagonal(dr, diag, y_within, y_across, z_within, z_across):
    ny, nz, width = diag.shape
    shift = 6.0 - CENTRE

    def put(y, z, row):
        dr[y, z] = jnp.broadcast_to(row + shift, (8, width))

    for y in range(ny):
        for z in range(nz):
            put(y + 2, z + 2, diag[y, z : z + 1])

    def y_sides(side_within, side_across):
        for got, side in ((y_within, side_within), (y_across, side_across)):
            start = 0 if side == 0 else ny + 2
            for layer in range(2):
                for z in range(nz):
                    row = layer * nz + z
                    put(start + layer, z + 2, got[row : row + 1])

    def z_sides(side_within, side_across):
        for got, side in ((z_within, side_within), (z_across, side_across)):
            start = 0 if side == 0 else nz + 2
            for y in range(ny + 4):
                for t in range(2):
                    put(y, start + t, got[2 * y + t : 2 * y + t + 1])

    when_sides("gy", y_sides)
    when_sides("gz", z_sides)


def sweep(source, ys, zs, at, emit, deep=2):
    parts = [pl.ds(h, 8) for h in range(0, source.shape[2], 8)]

    def rows(i, carry):
        def load(r, z):
            return [source[deep * i + (r + ys[0] + at), z + at, part] for part in parts]

        lines = range(deep)
        left = [load(r, zs[0] - 1) for r in lines]
        here = [load(r, zs[0]) for r in lines]
        for z in range(zs[0], zs[1]):
            right = [load(r, z + 1) for r in lines]
            column = [load(-1, z), *here, load(deep, z)]
            for r in lines:
                around = [
                    (column[r][n] + column[r + 2][n]) + (left[r][n] + right[r][n])
                    for n in range(len(parts))
                ]
                emit(deep * i + r, z, here[r], around)
            left, here = here, right
        return carry

    lax.fori_loop(0, (ys[1] - ys[0]) // deep, rows, 0)


def stencil(source, target, dr, ys, zs, source_at, target_at, seen=None, made=None, deep=2):
    width = source.shape[3]
    lane = lax.broadcasted_iota(jnp.int32, (8, width), 1)
    first, last = lane == 0, lane == width - 1

    def emit(row, z, heres, arounds):
        weight = dr[row + (ys[0] + 2), z + 2]
        values = []
        for here, around in zip(heres, arounds):
            left = jnp.where(first, 0.0, pltpu.roll(here, 1, 1))
            right = jnp.where(last, 0.0, pltpu.roll(here, width - 1, 1))
            values.append(weight * here - (around + (left + right)))
        if target is not None:
            for n, value in enumerate(values):
                target[row + (ys[0] + target_at), z + target_at, pl.ds(8 * n, 8)] = value
        if seen is not None:
            seen(row, z, heres)
        if made is not None:
            made(row, z, values)

    sweep(source, ys, zs, source_at, emit, deep)


def clear_edges(field, ny, nz, at, reach):
    y_low, y_high = edge("gy")
    z_low, z_high = edge("gz")
    for flag, y in ((y_low, -1), (y_high, ny)):

        @pl.when(flag)
        def _():
            for z in range(-reach, nz + reach):
                field[y + at, z + at] = jnp.zeros(field.shape[2:], field.dtype)

    for flag, z in ((z_low, -1), (z_high, nz)):

        @pl.when(flag)
        def _():
            for y in range(-reach, ny + reach):
                field[y + at, z + at] = jnp.zeros(field.shape[2:], field.dtype)


def weights_to_scalars(codes, z_within, z_across, table, marks, signs, places, sems, ny, nz):
    base = 2 * (ny + 4)
    z_low, z_high = edge("gz")
    low_within = odd("gz")
    a = z_within[base : base + 16]
    b = z_across[base : base + 16]
    low = jnp.where(z_low, 0.0, jnp.where(low_within, a, b))
    high = jnp.where(z_high, 0.0, jnp.where(low_within, b, a))
    lane = lax.broadcasted_iota(jnp.int32, (16, 128), 1)
    whole = jnp.where(
        lane < 3,
        low,
        jnp.where(
            lane < nz + 3,
            pltpu.roll(codes[...], 3, 1),
            jnp.where(lane < nz + 6, pltpu.roll(high, nz + 3, 1), 0.0),
        ),
    )
    table[...] = jnp.where(whole > 0, 1.0, jnp.where(whole < 0, -1.0, 0.0))
    marks[...] = jnp.maximum(jnp.abs(whole) - 1.0, 0.0).astype(jnp.int32)
    return [
        pltpu.make_async_copy(table, signs, sems.at[0]),
        pltpu.make_async_copy(marks, places, sems.at[1]),
    ]


def clear_rings(field, ny, nz, at, rings):
    blank = lambda n: jnp.zeros((n, *field.shape[2:]), field.dtype)
    inner, outer = rings
    for y in range(-outer, ny + outer):
        if y <= -inner or y >= ny - 1 + inner:
            field[y + at, at - outer : nz + at + outer] = blank(nz + 2 * outer)
        else:
            field[y + at, at - outer : at - inner + 1] = blank(outer - inner + 1)
            field[y + at, nz + at + inner - 1 : nz + at + outer] = blank(outer - inner + 1)


def local_sketches(
    vt, diag, code, y_within, y_across, z_within, z_across, gaussian, keep_out, give_out, dr,
    e0, e1, e2, table, marks, signs, places, sums, sums_a, sums_b, sums_c, sums_d, sems,
):
    ny, nz, width = diag.shape
    count = vt.shape[1]
    copies = weights_to_scalars(
        code, z_within, z_across, table, marks, signs, places, sems, ny, nz
    )
    for copy in copies:
        copy.start()
    spread_diagonal(dr, diag, y_within, y_across, z_within, z_across)
    clear_rings(e0, ny, nz, 2, (1, 2))
    clear_rings(e1, ny, nz, 3, (2, 3))
    clear_rings(e2, ny, nz, 4, (3, 4))
    for y in range(ny):
        e0[y + 2, 2 : 2 + nz] = vt[y * nz : (y + 1) * nz]
    for copy in copies:
        copy.wait()
    lanes = [sums_a, sums_b]
    above = [sums_c, sums_d]

    def added(refs, level):
        def add(row, z, values):
            sign = signs[row + (3 - level), z + 3]
            place = places[row + (3 - level), z + 3]
            ref = refs[z % 2]
            for n, value in enumerate(values):
                part = pl.ds(8 * n, 8)
                ref[place, part] = ref[place, part] + sign * value

        return add

    def clear(refs):
        for ref in refs:
            ref[...] = jnp.zeros_like(ref)

    def collect(level):
        for k in range(BUCKETS):
            sums[k, level * count : (level + 1) * count] = lanes[0][k] + lanes[1][k]

    clear(lanes)
    stencil(e0, e1, dr, (-1, ny + 1), (-1, nz + 1), 2, 3, added(lanes, 1))
    collect(0)
    clear_edges(e1, ny, nz, 3, 1)
    clear(lanes)
    stencil(e1, e2, dr, (-2, ny + 2), (-2, nz + 2), 3, 4, added(lanes, 2))
    collect(1)
    clear_edges(e2, ny, nz, 4, 2)
    clear(lanes)
    clear(above)
    outer = 3
    add_here, add_above = added(lanes, outer), added(above, outer)

    def emit(row, z, heres, arounds):
        at_y = jnp.clip(row + (2 - outer), 0, dr.shape[0] - 1)
        weight = dr[at_y, min(max(z + 2, 0), dr.shape[1] - 1)]
        add_here(row, z, heres)
        add_above(row, z, [weight * here - around for here, around in zip(heres, arounds)])

    sweep(e2, (-outer, ny + outer), (-outer, nz + outer), 4, emit)
    collect(2)
    last = [sums[k, 2 * count : 3 * count] for k in range(BUCKETS)]
    higher = [above[0][k] + above[1][k] for k in range(BUCKETS)]
    lane = lax.broadcasted_iota(jnp.int32, (count, width), 1)
    for k in range(BUCKETS):
        left = jnp.where(lane == 0, 0.0, pltpu.roll(last[k], 1, 1))
        right = jnp.where(lane == width - 1, 0.0, pltpu.roll(last[k], width - 1, 1))
        sums[k, 3 * count : 4 * count] = higher[k] - (left + right)
    rows = gaussian.shape[0] // BUCKETS

    def part(k):
        return lax.dot_general(
            sums[k],
            gaussian[k * rows : (k + 1) * rows],
            (((1,), (1,)), ((), ())),
            precision=HIGH,
            preferred_element_type=jnp.float32,
        )

    upper = odd("gy")
    size = (ITERS + 1) * count
    for k in range(BUCKETS // 2):
        one, two = part(k), part(k + BUCKETS // 2)
        keep_out[k * size : (k + 1) * size] = jnp.where(upper, two, one)
        give_out[k * size : (k + 1) * size] = jnp.where(upper, one, two)


CORNER = ((1, 1), (1, 2), (2, 1))


def pack_corners(y_within, y_across, after, within, across, nz):
    def act(side_within, side_across):
        for out, side in ((within, side_within), (across, side_across)):

            def corners(low, high):
                for n, (y, z) in enumerate(CORNER):
                    at = z - 1 if side == 0 else nz - z
                    out[n] = low[(3 - y) * nz + at]
                    out[len(CORNER) + n] = high[(y - 1) * nz + at]

            @pl.when(odd("gy"))
            def _():
                corners(y_within, y_across)

            @pl.when(jnp.logical_not(odd("gy")))
            def _():
                corners(y_across, y_within)

    when_sides("gz", act)


def split(field, at, high, low, ny, nz):
    def row(y, carry):
        for z in range(nz):
            value = field[y + at, z + at]
            top = value.astype(jnp.bfloat16)
            high[y * nz + z] = top
            low[y * nz + z] = (value - top.astype(jnp.float32)).astype(jnp.bfloat16)
        return carry

    lax.fori_loop(0, ny, row, 0)


def widened(
    vt, y_within, y_across, z_within, z_across, c_within, c_across, e0, high, low, ny, nz
):
    count, width = vt.shape[1:]
    for y in range(ny):
        e0[y + 3, 3 : 3 + nz] = vt[y * nz : (y + 1) * nz]
    y_edges, z_edges = edge("gy"), edge("gz")
    blank_y = jnp.zeros((nz, count, width), jnp.float32)
    blank_z = jnp.zeros((3, count, width), jnp.float32)

    def y_sides(side_within, side_across):
        for got, side in ((y_within, side_within), (y_across, side_across)):
            start = 0 if side == 0 else ny + 3
            for layer in range(3):
                e0[start + layer, 3 : 3 + nz] = got[layer * nz : (layer + 1) * nz]

            @pl.when(y_edges[side])
            def _():
                for layer in range(3):
                    e0[start + layer, 3 : 3 + nz] = blank_y

    def z_sides(side_within, side_across):
        for got, far, side in (
            (z_within, c_within, side_within), (z_across, c_across, side_across)
        ):
            start = 0 if side == 0 else nz + 3
            for y in range(ny):
                e0[y + 3, start : start + 3] = got[y]
            for layer in range(3):
                e0[layer, start : start + 3] = blank_z
                e0[ny + 3 + layer, start : start + 3] = blank_z
            for n, (y, z) in enumerate(CORNER):
                column = 3 - z if side == 0 else nz + 2 + z
                e0[3 - y, column] = far[n]
                e0[ny + 2 + y, column] = far[len(CORNER) + n]

            @pl.when(z_edges[side])
            def _():
                for y in range(ny + 6):
                    e0[y, start : start + 3] = blank_z

            for y_side in range(2):

                @pl.when(y_edges[y_side])
                def _():
                    for layer in range(3):
                        y = layer if y_side == 0 else ny + 3 + layer
                        e0[y, start : start + 3] = blank_z

    when_sides("gy", y_sides)
    when_sides("gz", z_sides)
    split(e0, 3, high, low, ny, nz)


def raised(source, dr, *outs, ny, nz, ring):
    *target, high, low = outs
    target = target[0] if target else None

    def made(row, z, values):
        if 0 <= z < nz:
            value = jnp.concatenate(values, axis=0)
            top = value.astype(jnp.bfloat16)
            high[row * nz + z] = top
            low[row * nz + z] = (value - top.astype(jnp.float32)).astype(jnp.bfloat16)

    def band(low_y, high_y, keep, deep):
        stencil(
            source, target, dr, (low_y, high_y), (-ring, nz + ring), ring + 1, ring,
            made=made if keep else None, deep=deep,
        )

    band(0, ny, True, 2)
    if ring > 0:
        band(-ring, 0, False, ring)
        band(ny, ny + ring, False, ring)
        clear_edges(target, ny, nz, ring, ring)


def product(a, b, axis):
    return lax.dot_general(
        a, b, (((1,), (axis,)), ((), ())), precision=HIGH, preferred_element_type=jnp.float32
    )


def factored(gram, block):
    count = gram.shape[0]
    width = 128
    columns = [jnp.broadcast_to(gram[:, j : j + 1], (count, width)) for j in range(count)]
    pieces = [block[:, c : c + width] for c in range(0, block.shape[1], width)]
    row = lax.broadcasted_iota(jnp.int32, (count, width), 0)
    lane = lax.broadcasted_iota(jnp.int32, (count, width), 1)
    lower = jnp.zeros((count, width), jnp.float32)
    scale = jnp.zeros((count, width), jnp.float32)
    for j in range(count):
        pivot = columns[j][j : j + 1]
        root = lax.rsqrt(pivot)
        inverse = root * root
        lower = jnp.where((lane == j) & (row >= j), columns[j] * root, lower)
        scale = jnp.where(row == j, jnp.broadcast_to(root, (count, width)), scale)
        under = jnp.where(row > j, columns[j] * inverse, 0.0)
        for m in range(j + 1, count):
            columns[m] = columns[m] - under * columns[m][j : j + 1]
        pieces = [piece - under * piece[j : j + 1] for piece in pieces]
    return lower, jnp.concatenate([piece * scale for piece in pieces], axis=1)


def finish(kept, got, *refs, ny, nz, scale):
    *halves, out, alphas, factors, block, out_sem = refs
    tops, bottoms = halves[0::2], halves[1::2]
    count = alphas.shape[1]
    size = (ITERS + 1) * count
    width = kept.shape[1]
    step = block.shape[1] // count
    upper = odd("gy")
    first = jnp.where(upper, got[...], kept[...])
    second = jnp.where(upper, kept[...], got[...])
    parts = [first[0:size], first[size:], second[0:size], second[size:]]
    whole = jnp.concatenate(parts, axis=1) * scale
    row = lax.broadcasted_iota(jnp.int32, (count, width), 0)
    lane = lax.broadcasted_iota(jnp.int32, (count, width), 1)
    identity = jnp.where(row == lane, 1.0, 0.0)
    start = whole[0:count]
    lower, current = factored(
        product(start, start, 1), jnp.concatenate([start, identity], axis=1)
    )
    previous = jnp.zeros_like(current)
    span = whole.shape[1]
    for number in range(ITERS):
        lifted = pltpu.roll(current[:, span:], count, 1)
        image_sketch = product(lifted[:, 0:size], whole, 0)
        image = jnp.concatenate([image_sketch, lifted], axis=1) + CENTRE * current
        both = jnp.concatenate([current, previous], axis=0)
        mixed = product(image[:, 0:span], both[:, 0:span], 1)
        alphas[number] = product(current[:, 0:span], image[:, 0:span], 1)
        residual = image - product(mixed, both, 0)
        previous = current
        sketch = residual[:, 0:span]
        lower, current = factored(product(sketch, sketch, 1), residual)
        factors[number] = lower[:, 0:count]
    mix = current[:, span : span + size]
    group = 4
    each = [mix[:, j * count : (j + 1) * count] for j in range(ITERS + 1)]
    tiled = jnp.concatenate([piece for piece in each for _ in range(group)], axis=1)
    tiled = jnp.concatenate([tiled] * group, axis=0)
    at_row = lax.broadcasted_iota(jnp.int32, tiled.shape, 0) // count
    at_lane = lax.broadcasted_iota(jnp.int32, tiled.shape, 1) // count % group
    tiled = jnp.where(at_row == at_lane, tiled, 0.0)
    mix_high = tiled.astype(jnp.bfloat16)
    mix_low = (tiled - mix_high.astype(jnp.float32)).astype(jnp.bfloat16)
    mix = jnp.concatenate([mix_high, mix_low], axis=0)

    def dot(a, b):
        return jnp.dot(a, b, preferred_element_type=jnp.float32)

    def copies(y):
        return [
            pltpu.make_async_copy(block.at[y, pl.ds(b * step, nz)], out.at[b, y], out_sem)
            for b in range(count)
        ]

    def layer(y, carry):
        for z in range(0, nz, group):
            col = y * nz + z
            pick = lambda ref: ref[pl.ds(col, group)].reshape(group * count, width)
            top = jnp.concatenate([pick(ref) for ref in tops], axis=0)
            bottom = jnp.concatenate([pick(ref) for ref in bottoms], axis=0)
            value = dot(mix, jnp.concatenate([top, bottom], axis=1))
            half = group * count
            value = value[:half, :width] + (value[:half, width:] + value[half:, :width])
            for c in range(group):
                block[y, pl.ds(z + c, count, stride=step), :] = value[c * count : (c + 1) * count]
        for copy in copies(y):
            copy.start()
        return carry

    lax.fori_loop(0, ny, layer, 0)

    def drain(y, carry):
        for copy in copies(y):
            copy.wait()
        return carry

    lax.fori_loop(0, ny, drain, 0)


def reduced(kept, given):
    ny, nz = lax.axis_size("gy"), lax.axis_size("gz")
    total = ny * nz

    def exchange(value, bit):
        return lax.ppermute(value, AXES, [(i, i ^ bit) for i in range(total)])

    bits = [1]
    bit = 2 * nz
    while bit < total:
        bits.append(bit)
        bit *= 2
    bit = 2
    while bit < nz:
        bits.append(bit)
        bit *= 2
    got = exchange(given, nz)
    half = after = kept + got
    for number, bit in enumerate(bits):
        got = exchange(half, bit)
        half = half + got
        after = after if number else half
    return half, exchange(half, nz), after


def iterated(start_block, diagonal, gaussian, bucket, flip):
    count, ny, nz, width = start_block.shape
    cells = width * ny * lax.axis_size("gy") * nz * lax.axis_size("gz")
    scale = 1.0 / math.sqrt(cells)
    f32, bf16 = jnp.float32, jnp.bfloat16
    size = (ITERS + 1) * count
    small_rows_y = 2 * nz + 8
    small_rows_z = 2 * (ny + 4) + 16
    tags = pltpu.VMEM(bucket.shape, bucket.dtype)
    plain = lambda value: pltpu.with_memory_space_constraint(value, HBM)
    diagonal, code, within, across = call(
        small_y,
        [
            (diagonal.shape, f32, VMEM), ((ny, 128), f32, VMEM),
            ((small_rows_y, width), f32, VMEM), ((small_rows_y, width), f32, VMEM),
        ],
        [HBM] * 3,
        [tags, tags, pltpu.SemaphoreType.DMA((3,))],
    )(plain(diagonal), plain(bucket), plain(flip))
    dy = swapped("gy", within, across)
    side = (3 * nz, count, width)
    z_side = (ny, 3, count, width)
    vt, y_within, y_across, z_within, z_across = call(
        functools.partial(turned, ny=ny, nz=nz),
        [((ny * nz, count, width), f32, VMEM)] + [(side, f32, VMEM)] * 2 + [(z_side, f32, VMEM)] * 2,
        [HBM],
        [pltpu.VMEM((ny, count * (nz + 8), width), f32), pltpu.SemaphoreType.DMA((ny,))],
        cost=WORK,
    )(plain(start_block))
    y_halo = swapped("gy", y_within, y_across)
    z_halo = swapped("gz", z_within, z_across)
    codes, within, across = call(
        small_z,
        [((16, 128), f32, VMEM), ((small_rows_z, width), f32, VMEM), ((small_rows_z, width), f32, VMEM)],
        [VMEM] * 4,
    )(diagonal, code, *dy)
    dz = swapped("gz", within, across)
    half = (BUCKETS // 2 * size, 128)
    field = lambda ring: pltpu.VMEM((ny + 2 * ring, nz + 2 * ring, count, width), f32)
    spread = (ny + 4, nz + 4, 8, width)
    kept, given, dr = call(
        local_sketches,
        [(half, f32, VMEM), (half, f32, VMEM), (spread, f32, VMEM)],
        [VMEM] * 8,
        [
            field(2), field(3), field(4),
            pltpu.VMEM((16, 128), f32), pltpu.VMEM((16, 128), jnp.int32),
            pltpu.SMEM((16, 128), f32), pltpu.SMEM((16, 128), jnp.int32),
            pltpu.VMEM((BUCKETS, size, width), f32),
            *[pltpu.VMEM((BUCKETS, count, width), f32)] * 4,
            pltpu.SemaphoreType.DMA((2,)),
        ],
        limit=28,
    )(vt, diagonal, codes, *dy, *dz, gaussian)
    kept, got, after = reduced(kept, given)
    corner = (2 * len(CORNER), count, width)
    corners = swapped(
        "gz",
        *call(
            functools.partial(pack_corners, nz=nz),
            [(corner, f32, VMEM), (corner, f32, VMEM)],
            [VMEM] * 3,
        )(*y_halo, after),
    )
    ring_shape = lambda ring: (ny + 2 * ring, nz + 2 * ring, count, width)
    half_type = ((ny * nz, count, width), bf16, VMEM)
    power, *halves = call(
        functools.partial(widened, ny=ny, nz=nz),
        [(ring_shape(3), f32, VMEM), half_type, half_type],
        [VMEM] * 7,
        limit=4,
        cost=WORK,
    )(vt, *y_halo, *z_halo, *corners)
    for ring in (2, 1, 0):
        field_type = [(ring_shape(ring), f32, VMEM)] if ring else []
        *field_out, high, low = call(
            functools.partial(raised, ny=ny, nz=nz, ring=ring),
            [*field_type, half_type, half_type],
            [VMEM] * 2,
            limit=4,
            cost=WORK,
        )(power, dr)
        power = field_out[0] if field_out else None
        halves += [high, low]
    square = (ITERS, count, count)
    basis, alphas, factors = call(
        functools.partial(finish, ny=ny, nz=nz, scale=scale),
        [(start_block.shape, f32, HBM), (square, f32, VMEM), (square, f32, VMEM)],
        [VMEM] * 10,
        [pltpu.VMEM((ny, count * (nz + 8), width), f32), pltpu.SemaphoreType.DMA],
        limit=12,
    )(kept, got, *halves)
    return basis, alphas, factors


def solution(mesh):
    in_specs = (P(None, "gy", "gz", None), P("gy", "gz", None), P(), P("gy", "gz"), P("gy", "gz"))
    out_specs = (P(None, "gy", "gz", None), P(), P())
    return jax.shard_map(
        iterated, mesh=mesh, in_specs=in_specs, out_specs=out_specs, check_vma=False
    )
```
